512 devices in a mesh: row: 32 (over x, y, core), col: 16 (over z).
Axes of the slice: x: 4, y: 4, z: 16, core: 2. Of those that a mesh axis runs over, the one named last changes fastest.
Arguments:
- history: float32 [3, 512, 65536], P(None, None, ('row', 'col')), may hold values from -8 to 8
Outputs:
- orbitals: float32 [512, 65536], P(None, ('row', 'col'))
The draws below stay inside these ranges and needn't reach their ends.
All inputs are finite; a program needn't handle non-finite values.
Results may differ from the reference program's by a relative error of at most 0.0003.
Values sent between devices are 32-bit elements; how exact they have to be, the bound alone decides.
A program may use at most 64 MiB of HBM per device.

```python
import jax
import jax.numpy as jnp
from jax import lax

NORB = 512
NHIST = 3
NPW = 65536


def draw_history(key, part):
    base_key = jax.random.fold_in(key, 11)
    base = jax.random.truncated_normal(base_key, -4.0, 4.0, (NORB, NPW), jnp.float32)
    drifts = jax.random.truncated_normal(jax.random.fold_in(key, 13), -4.0, 4.0, (NHIST, NORB, NPW), jnp.float32)
    return base[None, :, :] + 0.35 * drifts


def setup_inputs(seed: int = 0) -> dict:
    splits = jax.random.split(jax.random.key(seed), 2)
    history = draw_history(jax.random.fold_in(splits[1], 71), 0)
    return {"history": history}


def reference(history):
    precise = lax.Precision.HIGHEST
    npw_total = history.shape[2]
    newest = history[0]
    weights = (2.5, -2.0, 0.5)
    predicted = jnp.zeros(newest.shape, jnp.float32)
    for index in range(3):
        project = jnp.einsum('ip,jp->ij', newest, history[index], precision=precise) / npw_total
        predicted = predicted + weights[index] * jnp.dot(project, history[index], precision=precise)
    gram = jnp.einsum('ip,jp->ij', predicted, predicted, precision=precise) / npw_total
    factor = jnp.linalg.cholesky(gram)
    return lax.linalg.triangular_solve(factor, predicted, left_side=True, lower=True)
```

```python
import functools

import jax, jax.numpy as jnp
from jax import lax
from jax.experimental import pallas as pl
from jax.experimental.pallas import tpu as pltpu
from jax.sharding import PartitionSpec as P

NB = 12
f32, bf16 = jnp.float32, jnp.bfloat16
NN = (((1,), (0,)), ((), ()))
NT = (((1,), (1,)), ((), ()))
TN = (((0,), (0,)), ((), ()))


def split2(x):
    hi = x.astype(bf16)
    return hi, (x - hi.astype(f32)).astype(bf16)


def split3(x):
    hi = x.astype(bf16)
    rest = x - hi.astype(f32)
    mid = rest.astype(bf16)
    return hi, mid, (rest - mid.astype(f32)).astype(bf16)


def dot(a, b, dims):
    return lax.dot_general(a, b, dims, preferred_element_type=f32)


def dot3(ah, al, bh, bl, dims):
    return dot(ah, bh, dims) + (dot(ah, bl, dims) + dot(al, bh, dims))


def slot_of(i, b):
    d = (b - i) % NB
    if d <= 5:
        return 39 * (i // 6) + (i % 6) * 6 + d, False
    if d == 6 and i < 6:
        return 39 * (i // 3) + 36 + i % 3, False
    index, _ = slot_of(b, i)
    return index, True


def eliminate(aug, lhs, rhs, out, q, s):
    base = pl.multiple_of(q * 128, 128)
    r0 = pl.multiple_of(base + s * 32, 32)
    D = aug[pl.ds(r0, 32), pl.ds(base, 128)]
    C = []
    for j in range(32):
        lane = s * 32 + j
        C.append([None if t < j // 8 else jnp.broadcast_to(D[t * 8 : t * 8 + 8, lane : lane + 1], (8, 128)) for t in range(4)])
    R = [[aug[pl.ds(r0 + 8 * t, 8), pl.ds(128 * l, 128)] for l in range(5)] for t in range(4)]
    sub = lax.broadcasted_iota(jnp.int32, (8, 128), 0)
    scale = [jnp.zeros((8, 128), f32) for _ in range(4)]
    for j in range(32):
        tj, jj = j // 8, j % 8
        piv = jnp.broadcast_to(C[j][tj][jj : jj + 1, :], (8, 128))
        inv = 1.0 / piv
        scale[tj] = jnp.where(sub == jj, lax.rsqrt(piv), scale[tj])
        for m in range(j + 1, 32):
            sm = jnp.broadcast_to(C[j][m // 8][m % 8 : m % 8 + 1, :], (8, 128)) * inv
            for t in range(m // 8, 4):
                C[m][t] = C[m][t] - C[j][t] * sm
        for t in range(tj, 4):
            coef = C[j][t] * inv
            if t == tj:
                if jj == 7:
                    continue
                coef = jnp.where(sub > jj, coef, 0.0)
            for l in range(5):
                row = jnp.broadcast_to(R[tj][l][jj : jj + 1, :], (8, 128))
                R[t][l] = R[t][l] - coef * row
    U = jnp.concatenate([jnp.concatenate([R[t][l] * scale[t] for l in range(5)], axis=1) for t in range(4)], axis=0)
    out[pl.ds(r0, 32), :] = U[:, 512:]
    h, m, l = split3(U)
    for i, part in enumerate((h, m, h, l, h, m)):
        rhs[32 * i : 32 * i + 32, :] = part
    lane = lax.broadcasted_iota(jnp.int32, (32, 512), 1)
    h, m, l = split3(jnp.where(lane >= r0 + 32, U[:, :512], 0.0))
    for i, part in enumerate((h, h, m, h, l, m)):
        lhs[32 * i : 32 * i + 32, :] = part
    for v in range(4):
        top = 128 * v if s < 3 else 128 * (v + 1)
        if top == 512:
            continue

        @pl.when(q == v)
        def _():
            aug[top:, top:] = aug[top:, top:] - dot(lhs[:, top:], rhs[:, top:], TN)


def finish_kernel(n_total, s_ref, h_ref, out, ah, al, uh, ul, th, tl, aug, lhs, rhs):
    weights = (2.5, -2.0, 0.5)
    for i in range(4):
        for b in range(NB):
            index, flip = slot_of(i, b)
            block = s_ref[index]
            if flip:
                block = block.T
            hi, lo = split2(block * (weights[b // 4] / n_total))
            ah[i * 128 : i * 128 + 128, (b + 6) * 128 : (b + 7) * 128] = hi
            al[i * 128 : i * 128 + 128, (b + 6) * 128 : (b + 7) * 128] = lo
            if b >= 6:
                ah[i * 128 : i * 128 + 128, (b - 6) * 128 : (b - 5) * 128] = hi
                al[i * 128 : i * 128 + 128, (b - 6) * 128 : (b - 5) * 128] = lo
    zero = jnp.zeros((128, 128), bf16)
    for m in range(6):
        for k in range(8):
            i = 2 * m - 6 + k
            for e in range(2):
                qq = 2 * m + e
                d = qq - i
                at = (slice(k * 128, k * 128 + 128), slice(e * 128, e * 128 + 128))
                if d < 0 or d > 6 or (d == 6 and i < 0):
                    uh[at] = zero
                    ul[at] = zero
                    continue
                index, flip = slot_of(i % NB, qq)
                assert not flip
                hi, lo = split2(s_ref[index] * ((0.5 if d == 0 else 1.0) / n_total))
                uh[at] = hi
                ul[at] = lo
        span = slice(2 * m * 128, (2 * m + 8) * 128)
        t = dot3(ah[:, span], al[:, span], uh[...], ul[...], NN)
        hi, lo = split2(t)
        th[:, 256 * m : 256 * m + 256] = hi
        tl[:, 256 * m : 256 * m + 256] = lo
    half = dot3(th[...], tl[...], ah[:, 768:], al[:, 768:], NT)
    aug[:, :512] = half
    for i in range(4):
        for b in range(i, 4):
            one = aug[i * 128 : i * 128 + 128, b * 128 : b * 128 + 128]
            if b == i:
                aug[i * 128 : i * 128 + 128, b * 128 : b * 128 + 128] = one + one.T
            else:
                two = aug[b * 128 : b * 128 + 128, i * 128 : i * 128 + 128]
                both = one + two.T
                aug[i * 128 : i * 128 + 128, b * 128 : b * 128 + 128] = both
    xh, xl = split2(h_ref[...].reshape(1536, 128))
    aug[:, 512:] = dot3(ah[:, 768:], al[:, 768:], xh, xl, NN)

    @pl.loop(0, 4)
    def _(q):
        for s in range(4):
            eliminate(aug, lhs, rhs, out, q, s)


def finish(s, h, n_total):
    vm = pl.BlockSpec(memory_space=pltpu.VMEM)
    return pl.pallas_call(
        functools.partial(finish_kernel, n_total),
        out_shape=jax.ShapeDtypeStruct((512, 128), f32),
        in_specs=[vm, vm],
        out_specs=vm,
        scratch_shapes=[
            pltpu.VMEM((512, 18 * 128), bf16), pltpu.VMEM((512, 18 * 128), bf16),
            pltpu.VMEM((1024, 256), bf16), pltpu.VMEM((1024, 256), bf16),
            pltpu.VMEM((512, 1536), bf16), pltpu.VMEM((512, 1536), bf16),
            pltpu.VMEM((512, 640), f32), pltpu.VMEM((192, 512), bf16), pltpu.VMEM((192, 640), bf16),
        ],
        compiler_params=pltpu.CompilerParams(vmem_limit_bytes=56 * 1024 * 1024),
        name="finish",
    )(s, h)


PARTS = ((0, 10), (10, 10), (20, 10), (30, 9))
OWNERS = 13
MESH = pl.DeviceIdType.MESH


def reduce_kernel(h_ref, s_ref, hp, xh, xl, B, R0, R1, R2, R3, Z, ZF, RZ, xs, xr, rs, rr, gs, gr, zs, zr, ws, wr, cs, cr):
    row, z = lax.axis_index("row"), lax.axis_index("col")
    x, y, c = row // 8, (row // 2) % 4, row % 2

    def dev(x_, y_, c_, z_):
        return ((x_ * 4 + y_) * 2 + c_, z_)

    def copy(src, dst, send, recv, device):
        return pltpu.make_async_remote_copy(
            src_ref=src, dst_ref=dst, send_sem=send, recv_sem=recv, device_id=device, device_id_type=MESH
        )

    other = dev(x, y, 1 - c, z)
    low = lambda v: (v + v // 2) % 2
    flip_low = lambda v: v + 1 - 2 * (v % 2)
    dims = (
        (dev(flip_low(x), y, c, z), low(x)),
        (dev(x, flip_low(y), c, z), low(y)),
        (dev(3 - x, y, c, z), x // 2),
        (dev(x, 3 - y, c, z), y // 2),
    )
    zdev = [dev(x, y, c, (z + d) % 16) for d in range(16)]

    barrier = pltpu.get_barrier_semaphore()
    for device in [zdev[d] for d in (8, 7, 9, 6, 10, 5, 11, 4, 12, 3, 13, 2, 14, 1, 15)] + [p for p, _ in dims] + [other]:
        pl.semaphore_signal(barrier, inc=1, device_id=device, device_id_type=MESH)

    def place(rows, lanes, v):
        hi, lo = split2(v)
        xh[rows, lanes] = hi
        xl[rows, lanes] = lo

    own, far = slice(0, 128), slice(128, 256)
    for b in range(17):
        i = b % 12
        place(slice(128 * b, 128 * b + 128), own, h_ref[i // 4, 128 * (i % 4) : 128 * (i % 4) + 128, :])
    pl.semaphore_wait(barrier, 20)
    swap = copy(h_ref, hp, xs, xr, other)
    swap.start()
    swap.wait_recv()
    for b in range(17):
        i = b % 12
        place(slice(128 * b, 128 * b + 128), far, hp[i // 4, 128 * (i % 4) : 128 * (i % 4) + 128, :])

    offs = []
    for p in range(4):
        o, off = 0, [0]
        for s in range(4):
            o = o + dims[(p + s) % 4][1] * (64 >> s)
            off.append(pl.multiple_of(o, 64 >> s))
        offs.append(off)
    recvs = (R0, R1, R2, R3)

    def reduce_copy(p, s):
        lo, n = PARTS[p]
        partner, bit = dims[(p + s) % 4]
        half = 64 >> s
        start = pl.multiple_of(offs[p][s] + (1 - bit) * half, half)
        return copy(B.at[lo : lo + n, pl.ds(start, half), :], recvs[s].at[lo : lo + n], rs.at[p, s], rr.at[p, s], partner)

    def block_row(i, width):
        at = pl.ds(pl.multiple_of(i * 128, 128), 128)
        return at, pl.ds(pl.multiple_of(i * 128, 128), width * 128)

    for a in range(6):
        left, right = block_row(6 * c + a, 6)
        res = dot3(xh[left, :], xl[left, :], xh[right, :], xl[right, :], NT)
        for d in range(6):
            B[a * 6 + d] = res[:, 128 * d : 128 * d + 128]
        if a in (1, 3, 4):
            reduce_copy({1: 0, 3: 1, 4: 2}[a], 0).start()
    for a in range(3):
        left, _ = block_row(3 * c + a, 1)
        right, _ = block_row(3 * c + a + 6, 1)
        B[36 + a] = dot3(xh[left, :], xl[left, :], xh[right, :], xl[right, :], NT)
    reduce_copy(3, 0).start()

    for s in range(4):
        half = 64 >> s
        for p in range(4):
            lo, n = PARTS[p]
            blocks = slice(lo, lo + n)
            keep = pl.ds(offs[p][s + 1], half)
            reduce_copy(p, s).wait_recv()
            total = B[blocks, keep, :] + recvs[s][blocks]
            if s < 3:
                B[blocks, keep, :] = total
                reduce_copy(p, s + 1).start()
            else:
                Z[blocks] = total

    order = (8, 7, 9, 6, 10, 5, 11, 4, 12, 3, 13, 2, 14, 1, 15)

    def z_copy(d):
        k = (z + d) % 16
        return copy(Z.at[pl.ds(3 * k, 3)], RZ.at[d - 1], zs.at[d - 1], zr.at[d - 1], zdev[d])

    for d in order:
        @pl.when((z + d) % 16 < OWNERS)
        def _():
            z_copy(d).start()

    def w_copy(d):
        mine = ZF.at[pl.ds(3 * z, 3)]
        return copy(mine, mine, ws.at[d - 1], wr.at[d - 1], zdev[d])

    @pl.when(z < OWNERS)
    def _():
        total = Z[pl.ds(3 * z, 3)]
        for d in order[::-1]:
            copy(Z.at[0:3], RZ.at[d - 1], zs.at[d - 1], zr.at[d - 1], zdev[d]).wait_recv()
            total = total + RZ[d - 1]
        ZF[pl.ds(3 * z, 3)] = total
        for d in order:
            w_copy(d).start()

    for d in order[::-1]:
        k = (z + 16 - d) % 16

        @pl.when(k < OWNERS)
        def _():
            got = ZF.at[pl.ds(3 * k, 3)]
            copy(got, got, ws.at[d - 1], wr.at[d - 1], zdev[d]).wait_recv()

    def gather_copy(p, s):
        lo, n = PARTS[p]
        partner, _ = dims[(p + s) % 4]
        part = s_ref.at[pl.ds(39 * c + lo, n), pl.ds(offs[p][s + 1], 64 >> s), :]
        return copy(part, part, gs.at[p, s], gr.at[p, s], partner)

    def core_copy(p):
        lo, n = PARTS[p]
        part = s_ref.at[pl.ds(39 * c + lo, n)]
        return copy(part, part, cs.at[p], cr.at[p], other)

    for p in range(4):
        lo, n = PARTS[p]
        s_ref[pl.ds(39 * c + lo, n), pl.ds(offs[p][4], 8), :] = ZF[lo : lo + n]
        gather_copy(p, 3).start()
    for s in (3, 2, 1, 0):
        for p in range(4):
            gather_copy(p, s).wait_recv()
            if s:
                gather_copy(p, s - 1).start()
            else:
                core_copy(p).start()

    swap.wait_send()
    for p in range(4):
        for s in range(4):
            reduce_copy(p, s).wait_send()
            gather_copy(p, s).wait_send()
        core_copy(p).wait()
    for d in order:
        @pl.when((z + d) % 16 < OWNERS)
        def _():
            z_copy(d).wait_send()

        @pl.when(z < OWNERS)
        def _():
            w_copy(d).wait_send()


def reduce_all(h):
    vm = pl.BlockSpec(memory_space=pltpu.VMEM)
    dma = pltpu.SemaphoreType.DMA
    return pl.pallas_call(
        reduce_kernel,
        out_shape=jax.ShapeDtypeStruct((78, 128, 128), f32),
        in_specs=[vm],
        out_specs=vm,
        scratch_shapes=[
            pltpu.VMEM((3, 512, 128), f32),
            pltpu.VMEM((17 * 128, 256), bf16), pltpu.VMEM((17 * 128, 256), bf16),
            pltpu.VMEM((39, 128, 128), f32),
            pltpu.VMEM((39, 64, 128), f32), pltpu.VMEM((39, 32, 128), f32),
            pltpu.VMEM((39, 16, 128), f32), pltpu.VMEM((39, 8, 128), f32),
            pltpu.VMEM((39, 8, 128), f32), pltpu.VMEM((39, 8, 128), f32),
            pltpu.VMEM((15, 3, 8, 128), f32),
            dma, dma, dma((4, 4)), dma((4, 4)), dma((4, 4)), dma((4, 4)),
            dma((15,)), dma((15,)), dma((15,)), dma((15,)), dma((4,)), dma((4,)),
        ],
        compiler_params=pltpu.CompilerParams(
            collective_id=0, has_side_effects=True, vmem_limit_bytes=56 * 1024 * 1024
        ),
        name="reduce_all",
    )(h)


def solution(mesh):
    def on_device(history):
        n_total = float(history.shape[2] * mesh.size)
        return finish(reduce_all(history), history, n_total)

    both = ("row", "col")
    return jax.shard_map(
        on_device, mesh=mesh, in_specs=(P(None, None, both),), out_specs=P(None, both), check_vma=False
    )
```

```python
import functools

import jax
import jax.numpy as jnp
from jax import lax
from jax.experimental import pallas as pl
from jax.experimental.pallas import tpu as pltpu
from jax.sharding import PartitionSpec as P

f32, bf16 = jnp.float32, jnp.bfloat16
NN = (((1,), (0,)), ((), ()))
NT = (((1,), (1,)), ((), ()))
TN = (((0,), (0,)), ((), ()))
MESH = pl.DeviceIdType.MESH
WEIGHTS = (2.5, -2.0, 0.5)

RUNS = (
    ((0, 0), (1, 1), 11), ((0, 11), (2, 2), 1), ((3, 3), (2, 3), 9),
    ((4, 4), (5, 5), 7), ((4, 11), (6, 6), 1), ((7, 7), (6, 7), 5), ((8, 8), (9, 9), 3), ((8, 11), (10, 10), 1), ((11, 11), (10, 11), 1),
)
BLOCKS = tuple(
    tuple((run[core][0], run[core][1] + n) for run in RUNS for n in range(run[2])) for core in range(2)
)
CHUNKS = ((0, 13), (13, 13), (26, 13))
PARTS = ((0, 4), (4, 3), (7, 3), (10, 3))
ORDER = (8, 7, 9, 6, 10, 5, 11, 4, 12, 3, 13, 2, 14, 1, 15)


def split2(x):
    hi = x.astype(bf16)
    return hi, (x - hi.astype(f32)).astype(bf16)


def split3(x):
    hi = x.astype(bf16)
    rest = x - hi.astype(f32)
    mid = rest.astype(bf16)
    return hi, mid, (rest - mid.astype(f32)).astype(bf16)


def dot(a, b, dims):
    return lax.dot_general(a, b, dims, preferred_element_type=f32)


def dot3(ah, al, bh, bl, dims):
    return dot(ah, bh, dims) + (dot(ah, bl, dims) + dot(al, bh, dims))


def eliminate(aug, lhs, rhs, out, q, s):
    base = pl.multiple_of(q * 128, 128)
    r0 = pl.multiple_of(base + s * 32, 32)
    D = aug[pl.ds(r0, 32), pl.ds(base, 128)]
    C = []
    for j in range(32):
        lane = s * 32 + j
        C.append([None if t < j // 8 else jnp.broadcast_to(D[t * 8 : t * 8 + 8, lane : lane + 1], (8, 128)) for t in range(4)])
    R = [[aug[pl.ds(r0 + 8 * t, 8), pl.ds(128 * l, 128)] for l in range(5)] for t in range(4)]
    sub = lax.broadcasted_iota(jnp.int32, (8, 128), 0)
    scale = [jnp.zeros((8, 128), f32) for _ in range(4)]
    for j in range(32):
        tj, jj = j // 8, j % 8
        piv = jnp.broadcast_to(C[j][tj][jj : jj + 1, :], (8, 128))
        inv = 1.0 / piv
        scale[tj] = jnp.where(sub == jj, lax.rsqrt(piv), scale[tj])
        for m in range(j + 1, 32):
            sm = jnp.broadcast_to(C[j][m // 8][m % 8 : m % 8 + 1, :], (8, 128)) * inv
            for t in range(m // 8, 4):
                C[m][t] = C[m][t] - C[j][t] * sm
        for t in range(tj, 4):
            coef = C[j][t] * inv
            if t == tj:
                if jj == 7:
                    continue
                coef = jnp.where(sub > jj, coef, 0.0)
            for l in range(5):
                row = jnp.broadcast_to(R[tj][l][jj : jj + 1, :], (8, 128))
                R[t][l] = R[t][l] - coef * row
    U = jnp.concatenate([jnp.concatenate([R[t][l] * scale[t] for l in range(5)], axis=1) for t in range(4)], axis=0)
    out[pl.ds(r0, 32), :] = U[:, 512:]
    h, m, l = split3(U)
    for i, part in enumerate((h, m, h, l, h, m)):
        rhs[32 * i : 32 * i + 32, :] = part
    lane = lax.broadcasted_iota(jnp.int32, (32, 512), 1)
    h, m, l = split3(jnp.where(lane >= r0 + 32, U[:, :512], 0.0))
    for i, part in enumerate((h, h, m, h, l, m)):
        lhs[32 * i : 32 * i + 32, :] = part
    for v in range(4):
        top = 128 * v if s < 3 else 128 * (v + 1)
        if top == 512:
            continue

        @pl.when(q == v)
        def _():
            aug[top:, top:] = aug[top:, top:] - dot(lhs[:, top:], rhs[:, top:], TN)


def gram_kernel(
    n_total, h_ref, aug, hp, xh, xl, B, R0, R1, R2, R3, Z, ZF, RZ, S, ah, al, uh, ul, T, th, tl,
    xs, xr, rs, rr, gs, gr, zs, zr, ws, wr, cs, cr,
):
    row, z = lax.axis_index("row"), lax.axis_index("col")
    x, y, c = row // 8, (row // 2) % 4, row % 2

    def dev(x_, y_, c_, z_):
        return ((x_ * 4 + y_) * 2 + c_, z_)

    def copy(src, dst, send, recv, device):
        return pltpu.make_async_remote_copy(
            src_ref=src, dst_ref=dst, send_sem=send, recv_sem=recv, device_id=device, device_id_type=MESH
        )

    other = dev(x, y, 1 - c, z)
    low = lambda v: (v + v // 2) % 2
    flip_low = lambda v: v + 1 - 2 * (v % 2)
    dims = (
        (dev(flip_low(x), y, c, z), low(x)),
        (dev(x, flip_low(y), c, z), low(y)),
        (dev(3 - x, y, c, z), x // 2),
        (dev(x, 3 - y, c, z), y // 2),
    )
    zdev = [dev(x, y, c, (z + d) % 16) for d in range(16)]

    barrier = pltpu.get_barrier_semaphore()
    for device in [zdev[d] for d in ORDER] + [p for p, _ in dims] + [other]:
        pl.semaphore_signal(barrier, inc=1, device_id=device, device_id_type=MESH)

    def place(ref, lanes):
        for b in range(12):
            hi, lo = split2(ref[b // 4, 128 * (b % 4) : 128 * (b % 4) + 128, :])
            xh[128 * b : 128 * b + 128, lanes] = hi
            xl[128 * b : 128 * b + 128, lanes] = lo

    place(h_ref, slice(0, 128))
    for m in range(6):
        zero = jnp.zeros((128, 128), bf16)
        uh[(2 * m + 1) * 128 : (2 * m + 2) * 128, 2 * m * 128 : (2 * m + 1) * 128] = zero
        ul[(2 * m + 1) * 128 : (2 * m + 2) * 128, 2 * m * 128 : (2 * m + 1) * 128] = zero
    pl.semaphore_wait(barrier, 20)
    swap = copy(h_ref, hp, xs, xr, other)
    swap.start()
    swap.wait_recv()
    place(hp, slice(128, 256))

    offs = {}
    for r in range(4):
        o, off = 0, [0]
        for s in range(4):
            o = o + dims[(r + s) % 4][1] * (64 >> s)
            off.append(pl.multiple_of(o, 64 >> s))
        offs[r] = off
    recvs = (R0, R1, R2, R3)

    def part(k, p, s):
        lo, n = CHUNKS[k][0] + PARTS[p][0], PARTS[p][1]
        r = (p + k) % 4
        partner, bit = dims[(r + s) % 4]
        return lo, n, offs[r], partner, bit

    def reduce_copy(k, p, s):
        lo, n, off, partner, bit = part(k, p, s)
        half = 64 >> s
        start = pl.multiple_of(off[s] + (1 - bit) * half, half)
        return copy(
            B.at[lo : lo + n, pl.ds(start, half), :], recvs[s].at[lo : lo + n], rs.at[k, p, s], rr.at[k, p, s], partner
        )

    def gram(lo, hi):
        t = 0
        for first, second, count in RUNS:
            a, b = max(lo, t), min(hi, t + count)
            if a < b:
                i = first[0] + c * (second[0] - first[0])
                j = first[1] + c * (second[1] - first[1]) + (a - t)
                left = pl.ds(pl.multiple_of(i * 128, 128), 128)
                right = pl.ds(pl.multiple_of(j * 128, 128), (b - a) * 128)
                res = dot3(xh[left, :], xl[left, :], xh[right, :], xl[right, :], NT)
                for n in range(b - a):
                    B[a + n] = res[:, 128 * n : 128 * n + 128]
            t += count

    def start_reduce(k, s):
        for p in range(4):
            reduce_copy(k, p, s).start()

    def reduce_step(k, s):
        half = 64 >> s
        for p in range(4):
            lo, n, off, _, _ = part(k, p, s)
            blocks, keep = slice(lo, lo + n), pl.ds(off[s + 1], half)
            reduce_copy(k, p, s).wait_recv()
            total = B[blocks, keep, :] + recvs[s][blocks]
            if s < 3:
                B[blocks, keep, :] = total
                reduce_copy(k, p, s + 1).start()
            else:
                Z[blocks] = total

    def tile_of(k, z_):
        return (z_ + 5 * k) % 16

    def z_copy(k, d, tile):
        return copy(Z.at[13 * k + tile], RZ.at[k, d - 1], zs.at[k, d - 1], zr.at[k, d - 1], zdev[d])

    def w_copy(k, d, tile):
        mine = ZF.at[13 * k + tile]
        return copy(mine, mine, ws.at[k, d - 1], wr.at[k, d - 1], zdev[d])

    def z_start(k):
        for d in ORDER:
            tile = tile_of(k, z + d)

            @pl.when(tile < 13)
            def _():
                z_copy(k, d, tile).start()

    def z_step(k):
        mine = tile_of(k, z)

        @pl.when(mine < 13)
        def _():
            total = Z[13 * k + mine]
            for d in ORDER[::-1]:
                z_copy(k, d, 0).wait_recv()
                total = total + RZ[k, d - 1]
            ZF[13 * k + mine] = total
            for d in ORDER:
                w_copy(k, d, mine).start()

    def gather_copy(k, p, s):
        lo, n, off, partner, _ = part(k, p, s)
        piece = S.at[pl.ds(39 * c + lo, n), pl.ds(off[s + 1], 64 >> s), :]
        return copy(piece, piece, gs.at[k, p, s], gr.at[k, p, s], partner)

    def core_copy(k, p):
        lo, n, _, _, _ = part(k, p, 0)
        piece = S.at[pl.ds(39 * c + lo, n)]
        return copy(piece, piece, cs.at[k, p], cr.at[k, p], other)

    def z_end(k):
        for d in ORDER[::-1]:
            tile = tile_of(k, z + 16 - d)

            @pl.when(tile < 13)
            def _():
                w_copy(k, d, tile).wait_recv()

        for p in range(4):
            lo, n, off, _, _ = part(k, p, 3)
            S[pl.ds(39 * c + lo, n), pl.ds(off[4], 8), :] = ZF[lo : lo + n]
            gather_copy(k, p, 3).start()

    def gather_step(k, s):
        for p in range(4):
            gather_copy(k, p, s).wait_recv()
            if s:
                gather_copy(k, p, s - 1).start()
            else:
                core_copy(k, p).start()

    def core_end(k):
        for p in range(4):
            core_copy(k, p).wait_recv()

    def take(k):
        for t in range(CHUNKS[k][0], CHUNKS[k][0] + CHUNKS[k][1]):
            for core in range(2):
                i, b = BLOCKS[core][t]
                rows, lanes = slice(i * 128, i * 128 + 128), slice(b * 128, b * 128 + 128)
                block = S[39 * core + t]
                uh[rows, lanes], ul[rows, lanes] = split2(block * ((0.5 if i == b else 1.0) / n_total))
                if i < 4:
                    scaled = block * (WEIGHTS[b // 4] / n_total)
                    ah[rows, lanes], al[rows, lanes] = split2(scaled)
                    if i < b < 4:
                        ah[lanes, rows], al[lanes, rows] = split2(scaled.T)

    gram(0, 13)
    start_reduce(0, 0)
    gram(13, 26)
    start_reduce(1, 0)
    gram(26, 39)
    reduce_step(0, 0)
    start_reduce(2, 0)
    for k, s in ((1, 0), (0, 1), (2, 0), (1, 1), (0, 2), (2, 1), (1, 2)):
        reduce_step(k, s)
    reduce_step(0, 3)
    z_start(0)
    reduce_step(2, 2)
    reduce_step(1, 3)
    z_start(1)
    reduce_step(2, 3)
    z_start(2)
    z_step(0)
    z_step(1)
    z_step(2)
    z_end(0)
    gather_step(0, 3)
    z_end(1)
    gather_step(0, 2)
    gather_step(1, 3)
    z_end(2)
    for k, s in ((0, 1), (1, 2), (2, 3), (0, 0), (1, 1), (2, 2)):
        gather_step(k, s)
    core_end(0)
    take(0)
    gather_step(1, 0)
    gather_step(2, 1)
    core_end(1)
    take(1)
    gather_step(2, 0)
    aug[:, 512:] = dot3(ah[...], al[...], xh[:, :128], xl[:, :128], NN)
    for m in range(6):
        depth, lanes = slice(0, min(256 * m + 256, 512)), slice(256 * m, 256 * m + 256)
        t = dot3(ah[:, depth], al[:, depth], uh[depth, lanes], ul[depth, lanes], NN)
        if m < 2:
            th[:, lanes], tl[:, lanes] = split2(t)
        else:
            T[:, lanes] = t
    core_end(2)
    take(2)
    for m in range(2, 6):
        depth, lanes = slice(512, 256 * m + 256), slice(256 * m, 256 * m + 256)
        t = T[:, lanes] + dot3(ah[:, depth], al[:, depth], uh[depth, lanes], ul[depth, lanes], NN)
        th[:, lanes], tl[:, lanes] = split2(t)
    aug[:, :512] = dot3(th[...], tl[...], ah[...], al[...], NT)
    for i in range(4):
        for b in range(i, 4):
            at = slice(i * 128, i * 128 + 128), slice(b * 128, b * 128 + 128)
            aug[at] = aug[at] + aug[at[1], at[0]].T

    swap.wait_send()
    for k in range(3):
        for p in range(4):
            for s in range(4):
                reduce_copy(k, p, s).wait_send()
                gather_copy(k, p, s).wait_send()
            core_copy(k, p).wait_send()
        for d in ORDER:
            tile = tile_of(k, z + d)

            @pl.when(tile < 13)
            def _():
                z_copy(k, d, tile).wait_send()

        mine = tile_of(k, z)

        @pl.when(mine < 13)
        def _():
            for d in ORDER:
                w_copy(k, d, mine).wait_send()


def solve_kernel(aug_ref, out, aug, lhs, rhs):
    aug[...] = aug_ref[...]

    @pl.loop(0, 4)
    def _(q):
        for s in range(4):
            eliminate(aug, lhs, rhs, out, q, s)


def on_device(n_total, h):
    vm = pl.BlockSpec(memory_space=pltpu.VMEM)
    dma = pltpu.SemaphoreType.DMA
    wide = lambda *shape: pltpu.VMEM(shape, f32)
    narrow = lambda *shape: pltpu.VMEM(shape, bf16)
    aug = pl.pallas_call(
        functools.partial(gram_kernel, n_total),
        out_shape=jax.ShapeDtypeStruct((512, 640), f32),
        in_specs=[vm],
        out_specs=vm,
        scratch_shapes=[
            wide(3, 512, 128), narrow(1536, 256), narrow(1536, 256), wide(39, 128, 128),
            wide(39, 64, 128), wide(39, 32, 128), wide(39, 16, 128), wide(39, 8, 128),
            wide(39, 8, 128), wide(39, 8, 128), wide(3, 15, 8, 128), wide(78, 128, 128),
            narrow(512, 1536), narrow(512, 1536), narrow(1536, 1536), narrow(1536, 1536),
            wide(512, 1536), narrow(512, 1536), narrow(512, 1536),
            dma, dma, dma((3, 4, 4)), dma((3, 4, 4)), dma((3, 4, 4)), dma((3, 4, 4)),
            dma((3, 15)), dma((3, 15)), dma((3, 15)), dma((3, 15)), dma((3, 4)), dma((3, 4)),
        ],
        compiler_params=pltpu.CompilerParams(
            collective_id=0, has_side_effects=True, vmem_limit_bytes=56 * 1024 * 1024
        ),
        name="gram",
    )(h)
    return pl.pallas_call(
        solve_kernel,
        out_shape=jax.ShapeDtypeStruct((512, 128), f32),
        in_specs=[vm],
        out_specs=vm,
        scratch_shapes=[wide(512, 640), narrow(192, 512), narrow(192, 640)],
        compiler_params=pltpu.CompilerParams(vmem_limit_bytes=32 * 1024 * 1024),
        name="solve",
    )(aug)


def solution(mesh):
    both = ("row", "col")
    n_total = 128.0 * mesh.size
    return jax.shard_map(
        functools.partial(on_device, n_total),
        mesh=mesh, in_specs=(P(None, None, both),), out_specs=P(None, both), check_vma=False,
    )
```
